32 devices in a mesh: bx: 8 (over y, x, core), by: 4 (over z).
Axes of the slice: x: 2, y: 2, z: 4, core: 2. Of those that a mesh axis runs over, the one named last changes fastest.
Arguments:
- photon_data: float32 [6, 512, 128, 128], P(None, 'bx', 'by'), may hold values from 0 to 1, as said below
- block_counts: int32 [512, 128], P('bx', 'by'), may hold values from 1 to 128
- gather_offsets: float32 [3, 131072], P(None, ('bx', 'by')), may hold values from 0 to 1, as said below
- gather_blocks: int32 [4, 131072], P(None, ('bx', 'by')), may hold values from 0 to 65535, as said below
- albedo: float32 [3, 131072], P(None, ('bx', 'by')), may hold values from 0.1 to 1
- gather_pixels: int32 [131072], P(('bx', 'by')), may hold values from 0 to 65535, as said below
- tile_slot: int32 [256], replicated, may hold values from 0 to 255, as said below
Outputs:
- film: float32 [3, 256, 256], P(None, ('bx', 'by'))
The draws below stay inside these ranges and needn't reach their ends.
Inputs may be any that keep to these rules, and one draw needn't show every extreme that they name: `photon_data`: per point and channel in cell units: entries 0 to 2 are a position in [0, 1), entries 3 to 5 a positive power. `gather_offsets`: each coordinate lies in [0, 1). `gather_blocks`: entry 0 is the point's own cell, inside the brick of the device that holds the point; the 4 entries are the four different cells of a 2 x 2 square of cells (periodic) that contains it. `gather_pixels`: in the rows of one device, at most 384 gather points lie in tiles whose slots s share s // 8; in every draw some such owner group receives exactly 384 from every device. `tile_slot`: A permutation of 0 to 255.
All inputs are finite; a program needn't handle non-finite values.
Results may differ from the reference program's by a relative error of at most 0.0003.
Values sent between devices are 32-bit elements; how exact they have to be, the bound alone decides.
A program may use at most 512 MiB of HBM per device.

```python
import math
import jax
import jax.numpy as jnp
from jax import lax

CX = 64
CY = 32
SLOTS = 128
LISTED = 4
G_DEV = 4096
TILE_PIX = 256
TILE_DEV = 8
OWNERS = 32
NXC = 512
NYC = 128
NG = 131072
TILES = 256
CAP = 384


def gather_geometry(key):
    base = jax.random.fold_in(key, 11)
    keys = jax.random.split(base, 5)
    rows = jnp.arange(NG, dtype=jnp.int32)
    device = rows // G_DEV
    bricks_y = NYC // CY
    home_x = device // bricks_y * CX + jax.random.randint(keys[0], (NG,), 0, CX)
    home_y = device % bricks_y * CY + jax.random.randint(keys[1], (NG,), 0, CY)
    step_x = 2 * jax.random.randint(keys[2], (NG,), 0, 2) - 1
    step_y = 2 * jax.random.randint(keys[3], (NG,), 0, 2) - 1
    turn = jax.random.randint(keys[4], (NG,), 0, 3)
    return (home_x, home_y, step_x, step_y, turn)


def owner_plan(key):
    base = jax.random.fold_in(key, 23)
    keys = jax.random.split(base, 5)
    perm = jax.random.permutation(keys[0], TILES).astype(jnp.int32)
    pool = OWNERS * CAP
    heavy = jax.random.randint(keys[1], (), 0, OWNERS)
    owner_of = jnp.arange(pool, dtype=jnp.int32) // CAP

    def one_device(dev_key):
        scores = jax.random.permutation(dev_key, pool).astype(jnp.int32)
        order = jnp.argsort(jnp.where(owner_of == heavy, 0, pool) + scores, stable=True)
        picked = order[:G_DEV] // CAP
        mixing = jax.random.permutation(jax.random.fold_in(dev_key, 1), G_DEV)
        return picked[mixing].astype(jnp.int32)
    dev_keys = jax.vmap(lambda d: jax.random.fold_in(keys[2], d))(jnp.arange(OWNERS))
    owner = jax.vmap(one_device)(dev_keys).reshape(NG)
    local_tile = jax.random.randint(keys[3], (NG,), 0, TILE_DEV)
    slot = owner * TILE_DEV + local_tile
    inverse = jnp.argsort(perm, stable=True).astype(jnp.int32)
    tile = inverse[slot]
    pixel = tile * TILE_PIX + jax.random.randint(keys[4], (NG,), 0, TILE_PIX)
    return (perm, pixel.astype(jnp.int32))


def draw_tile_slot(key, part):
    return owner_plan(key)[0]


def draw_gather_pixels(key, part):
    return owner_plan(key)[1]


def draw_gather_blocks(key, part):
    home_x, home_y, step_x, step_y, turn = gather_geometry(key)
    own = home_x * NYC + home_y
    beside_x = (home_x + step_x) % NXC * NYC + home_y
    beside_y = home_x * NYC + (home_y + step_y) % NYC
    beside_xy = (home_x + step_x) % NXC * NYC + (home_y + step_y) % NYC
    others = jnp.stack([beside_x, beside_y, beside_xy])
    picks = []
    for entry in range(3):
        which = (entry + turn) % 3
        picks.append(jnp.where(which == 0, others[0], jnp.where(which == 1, others[1], others[2])))
    return jnp.stack([own] + picks).astype(jnp.int32)


def draw_gather_offsets(key, part):
    home_x, home_y, step_x, step_y, turn = gather_geometry(key)
    uniforms = jax.random.uniform(jax.random.fold_in(key, 12), (3, NG), jnp.float32, 0.0, 0.999)
    off_x = jnp.where(step_x > 0, 0.5 + 0.49 * uniforms[0], 0.5 - 0.5 * uniforms[0])
    off_y = jnp.where(step_y > 0, 0.5 + 0.49 * uniforms[1], 0.5 - 0.5 * uniforms[1])
    return jnp.stack([off_x, off_y, uniforms[2]]).astype(jnp.float32)


def draw_photon_data(key, part):
    keys = jax.random.split(jax.random.fold_in(key, 31), 2)
    places = jax.random.uniform(keys[0], (3, NXC, NYC, SLOTS), jnp.float32, 0.0, 0.999)
    log_power = jax.random.uniform(keys[1], (3, NXC, NYC, SLOTS), jnp.float32, jnp.log(0.02), jnp.log(0.2))
    power = jnp.exp(log_power)
    return jnp.concatenate([places, power], axis=0).astype(jnp.float32)


def place_ends(result, rng, smallest, largest):
    longest = result.shape.index(max(result.shape))
    spots = []
    for shift in (0, 1):
        where = [jax.random.randint(jax.random.fold_in(rng, axis), (), 0, length) for axis, length in enumerate(result.shape)]
        where[longest] = (where[longest] + shift) % result.shape[longest]
        spots.append(tuple(where))
    return result.at[spots[0]].set(smallest).at[spots[1]].set(largest)


def block_scale(own_key, dims, cuts, low, largest):
    factor_of, own = 1.0, jax.random.fold_in(own_key, 6)
    for position, blocks in cuts:
        draws = jnp.exp(jax.random.uniform(jax.random.fold_in(own, position), (blocks,), jnp.float32, low / len(cuts), largest / len(cuts)))
        factor_of = factor_of * jnp.repeat(draws, dims[position] // blocks).reshape([-1 if axis == position else 1 for axis in range(len(dims))])
    return factor_of


def setup_inputs(seed: int = 0) -> dict:
    splits = jax.random.split(jax.random.key(seed), 8)
    return {
        "photon_data": draw_photon_data(jax.random.fold_in(splits[7], 71), 0),
        "block_counts": place_ends(jax.random.randint(splits[1], (NXC, NYC), 1, SLOTS + 1), jax.random.fold_in(splits[1], 1), 1, SLOTS).astype(jnp.int32),
        "gather_offsets": draw_gather_offsets(jax.random.fold_in(splits[7], 71), 0),
        "gather_blocks": draw_gather_blocks(jax.random.fold_in(splits[7], 71), 0),
        "albedo": jnp.clip(jnp.exp(math.log(1.0) - 2.3025851 * jax.random.uniform(splits[4], (3, NG), jnp.float32) ** block_scale(splits[4], (3, NG), ((1, 32),), -0.2, 0.2)), 0.1, 1.0),
        "gather_pixels": draw_gather_pixels(jax.random.fold_in(splits[7], 71), 0),
        "tile_slot": draw_tile_slot(jax.random.fold_in(splits[7], 71), 0),
    }


RADIUS_SQ = 0.25


def kernel_sum(blocks, live, shift_x, shift_y, offsets, albedo):
    delta_x = (shift_x[:, :, None] + blocks[0]) - offsets[0][:, None, None]
    delta_y = (shift_y[:, :, None] + blocks[1]) - offsets[1][:, None, None]
    delta_z = blocks[2] - offsets[2][:, None, None]
    dist_sq = delta_x * delta_x + delta_y * delta_y + delta_z * delta_z
    weight = jnp.maximum(1.0 - dist_sq / RADIUS_SQ, 0.0)
    weight = jnp.where(live, weight, 0.0)
    sums = jnp.sum(weight[None] * blocks[3:6], axis=(2, 3))
    return albedo * sums


def reference(photon_data, block_counts, gather_offsets, gather_blocks, albedo, gather_pixels, tile_slot):
    slots = photon_data.shape[3]
    table = photon_data.reshape(6, NXC * NYC, slots)
    count_table = block_counts.reshape(NXC * NYC)
    group = math.gcd(NG, 4096)
    groups = NG // group
    ids = gather_blocks.reshape(LISTED, groups, group).transpose(1, 2, 0)
    offs = gather_offsets.reshape(3, groups, group).transpose(1, 0, 2)
    albs = albedo.reshape(3, groups, group).transpose(1, 0, 2)

    def one_group(packed):
        idb, off, alb = packed
        cell_x = idb // NYC
        cell_y = idb % NYC
        shift_x = ((cell_x - cell_x[:, :1] + 1) % NXC - 1).astype(jnp.float32)
        shift_y = ((cell_y - cell_y[:, :1] + 1) % NYC - 1).astype(jnp.float32)
        flat = idb.reshape(-1)
        blocks = jnp.take(table, flat, axis=1).reshape(6, group, LISTED, slots)
        counts = jnp.take(count_table, flat).reshape(group, LISTED)
        live = jnp.arange(slots, dtype=jnp.int32)[None, None, :] < counts[:, :, None]
        return kernel_sum(blocks, live, shift_x, shift_y, off, alb)

    rad = lax.map(one_group, (ids, offs, albs))
    radiance = rad.transpose(1, 0, 2).reshape(3, NG)
    tile = gather_pixels // TILE_PIX
    slot = jnp.take(tile_slot, tile)
    target = slot * TILE_PIX + gather_pixels % TILE_PIX
    film = jnp.zeros((3, TILES * TILE_PIX), jnp.float32).at[:, target].add(radiance)
    return film.reshape(3, TILES, TILE_PIX)
```

```python
import functools

import jax
import jax.numpy as jnp
from jax import lax
from jax.experimental import pallas as pl
from jax.experimental.pallas import tpu as pltpu
from jax.sharding import PartitionSpec as P

TILE_PIX = 256
INV_RADIUS_SQ = 4.0
FAR = 1.0e4
LANES = 128
MESH = pl.DeviceIdType.MESH
HIGHEST = lax.Precision.HIGHEST
NT = (((1,), (1,)), ((), ()))
GROUP = 32


def halo_kernel(nx, ny, cx, cy, send, recv, send_sem, recv_sem):
    ix, iy = lax.axis_index("bx"), lax.axis_index("by")
    right, left = lax.rem(ix + 1, nx), lax.rem(ix + nx - 1, nx)
    up, down = lax.rem(iy + 1, ny), lax.rem(iy + ny - 1, ny)
    peers = [
        (right, iy, 0, cy),
        (left, iy, cy, cy),
        (ix, up, 2 * cy, cx),
        (ix, down, 2 * cy + cx, cx),
        (right, up, 2 * cy + 2 * cx, 8),
        (right, down, 2 * cy + 2 * cx + 8, 8),
        (left, up, 2 * cy + 2 * cx + 16, 8),
        (left, down, 2 * cy + 2 * cx + 24, 8),
    ]
    barrier = pltpu.get_barrier_semaphore()
    for px, py, _, _ in peers:
        pl.semaphore_signal(barrier, inc=1, device_id=(px, py), device_id_type=MESH)
    pl.semaphore_wait(barrier, len(peers))
    copies = []
    for n, (px, py, first, rows) in enumerate(peers):
        part = pl.ds(first, rows)
        copies.append(
            pltpu.make_async_remote_copy(
                src_ref=send.at[:, part],
                dst_ref=recv.at[:, part],
                send_sem=send_sem.at[n],
                recv_sem=recv_sem.at[n],
                device_id=(px, py),
                device_id_type=MESH,
            )
        )
    for n in (2, 3, 0, 1, 4, 5, 6, 7):
        copies[n].start()
    for copy in copies:
        copy.wait()


def exchange_halo(send, nx, ny, cx, cy):
    return pl.pallas_call(
        functools.partial(halo_kernel, nx, ny, cx, cy),
        out_shape=jax.ShapeDtypeStruct(send.shape, jnp.float32),
        in_specs=[pl.BlockSpec(memory_space=pl.ANY)],
        out_specs=pl.BlockSpec(memory_space=pl.ANY),
        scratch_shapes=[pltpu.SemaphoreType.DMA((8,)), pltpu.SemaphoreType.DMA((8,))],
        compiler_params=pltpu.CompilerParams(collective_id=0, has_side_effects=True),
        name="halo",
    )(send)


def radiance_kernel(
    cells, rows, owners, cap_rows,
    idx, pts, alb, meta, first, rest, halo, out,
    table, stage, cols, acc, packed, tri, sems,
):
    listed = 4
    points = pts.shape[1]
    fills = [
        pltpu.make_async_copy(first, table.at[pl.ds(0, cells)], sems.at[0]),
    ]
    for c in range(1, 6):
        fills.append(
            pltpu.make_async_copy(rest.at[c], table.at[pl.ds(c * rows, cells)], sems.at[c])
        )
    for c in range(6):
        fills.append(
            pltpu.make_async_copy(
                halo.at[c], table.at[pl.ds(c * rows + cells, rows - cells)], sems.at[6 + c]
            )
        )
    for fill in fills:
        fill.start()
    a = lax.broadcasted_iota(jnp.int32, (LANES, LANES), 0)
    b = lax.broadcasted_iota(jnp.int32, (LANES, LANES), 1)
    tri[...] = jnp.where(a < b, 1.0, 0.0).astype(jnp.bfloat16)
    packed[...] = jnp.zeros_like(packed)
    for fill in fills:
        fill.wait()
    ones = jnp.ones((8, LANES), jnp.float32)
    own_iota = lax.broadcasted_iota(jnp.int32, (owners, LANES), 0)
    cap_iota = lax.broadcasted_iota(jnp.int32, (cap_rows * LANES, LANES), 0).astype(jnp.float32)

    def block(blk, carry):
        base = pl.multiple_of(blk * LANES, LANES)
        span = pl.ds(base, LANES)
        cols[...] = pts[:, span].T

        def some(sub, _):
            start = sub * GROUP
            for p in range(GROUP):
                for k in range(listed):
                    row = idx[k * points + base + start + p]
                    stage[pl.ds(k * 6 * GROUP + p, 6, stride=GROUP), :] = table[
                        pl.ds(row, 6, stride=rows), :
                    ]
            for q in range(GROUP // 8):
                place = pl.ds(pl.multiple_of(start + q * 8, 8), 8)
                col = cols[place, :]
                oz = jnp.broadcast_to(col[:, 8:9], (8, LANES))
                totals = [None] * 3
                for k in range(listed):
                    def chan(c):
                        return stage[pl.ds((k * 6 + c) * GROUP + q * 8, 8), :]
                    dx = chan(0) - jnp.broadcast_to(col[:, k : k + 1], (8, LANES))
                    dy = chan(1) - jnp.broadcast_to(col[:, 4 + k : 5 + k], (8, LANES))
                    dz = chan(2) - oz
                    d2 = dx * dx + dy * dy + dz * dz
                    w = jnp.maximum(1.0 - d2 * INV_RADIUS_SQ, 0.0)
                    for c in range(3):
                        term = w * chan(3 + c)
                        totals[c] = term if k == 0 else totals[c] + term
                for c in range(3):
                    acc[c, place, :] = totals[c]
            return 0

        lax.fori_loop(0, LANES // GROUP, some, 0)
        own = meta[0:1, span]
        mine = own_iota == own
        hot = jnp.where(mine, 1.0, 0.0)
        before = jnp.dot(hot.astype(jnp.bfloat16), tri[...], preferred_element_type=jnp.float32)
        rank = jnp.sum(jnp.where(mine, before + carry, 0.0), axis=0, keepdims=True)
        values = []
        for c in range(3):
            sums = lax.dot_general(
                ones, acc[c], NT, precision=HIGHEST, preferred_element_type=jnp.float32
            )
            rad = sums[0:1] * alb[c : c + 1, span]
            high = rad.astype(jnp.bfloat16).astype(jnp.float32)
            values += [high, rad - high]
        values += [meta[1:2, span].astype(jnp.float32), meta[2:3, span].astype(jnp.float32)]
        left = jnp.concatenate(
            [jnp.where(mine, v, 0.0).astype(jnp.bfloat16) for v in values], axis=0
        )
        right = jnp.where(cap_iota == rank, 1.0, 0.0).astype(jnp.bfloat16)
        packed[...] += lax.dot_general(left, right, NT, preferred_element_type=jnp.float32)
        return carry + jnp.sum(hot, axis=1, keepdims=True)

    lax.fori_loop(0, points // LANES, block, jnp.zeros((owners, 1), jnp.float32))
    pitch = out.shape[0] // owners

    def part(v, j):
        return packed[pl.ds(v * owners, owners), pl.ds(j * LANES, LANES)]

    for j in range(cap_rows):
        for c in range(3):
            out[pl.ds(c * cap_rows + j, owners, stride=pitch), :] = part(2 * c, j) + part(2 * c + 1, j)
        out[pl.ds(3 * cap_rows + j, owners, stride=pitch), :] = part(6, j)
        out[pl.ds(4 * cap_rows + j, owners, stride=pitch), :] = part(7, j)
    for r in range(5 * cap_rows, pitch):
        out[pl.ds(r, owners, stride=pitch), :] = jnp.zeros((owners, LANES), jnp.float32)


def pack_radiance(idx, pts, alb, meta, first, photons, halo, owners, cap_rows):
    cells = first.shape[0]
    rows = cells + halo.shape[1]
    pitch = -(-5 * cap_rows // 8) * 8
    vm = pl.BlockSpec(memory_space=pltpu.VMEM)
    hb = pl.BlockSpec(memory_space=pl.ANY)
    return pl.pallas_call(
        functools.partial(radiance_kernel, cells, rows, owners, cap_rows),
        out_shape=jax.ShapeDtypeStruct((owners * pitch, LANES), jnp.float32),
        in_specs=[pl.BlockSpec(memory_space=pltpu.SMEM), vm, vm, vm, hb, hb, hb],
        out_specs=vm,
        scratch_shapes=[
            pltpu.VMEM((6 * rows, LANES), jnp.float32),
            pltpu.VMEM((4 * 6 * GROUP, LANES), jnp.float32),
            pltpu.VMEM((LANES, pts.shape[0]), jnp.float32),
            pltpu.VMEM((3, LANES, LANES), jnp.float32),
            pltpu.VMEM((8 * owners, cap_rows * LANES), jnp.float32),
            pltpu.VMEM((LANES, LANES), jnp.bfloat16),
            pltpu.SemaphoreType.DMA((12,)),
        ],
        name="radiance",
    )(idx, pts, alb, meta, first, photons, halo)


def film_kernel(nx, ny, cap_rows, unroll, send, out, recv, send_sem, recv_sem, own_sem):
    count = nx * ny
    ix, iy = lax.axis_index("bx"), lax.axis_index("by")
    me = ix * ny + iy
    barrier = pltpu.get_barrier_semaphore()

    def greet(s, _):
        to = lax.rem(me + s, count)
        pl.semaphore_signal(
            barrier, inc=1, device_id=(to // ny, lax.rem(to, ny)), device_id_type=MESH
        )
        return 0

    lax.fori_loop(1, count, greet, 0)
    own = pltpu.make_async_copy(send.at[me], recv.at[me], own_sem)
    own.start()
    pl.semaphore_wait(barrier, count - 1)

    def copy_to(s):
        to = lax.rem(me + s, count)
        return pltpu.make_async_remote_copy(
            src_ref=send.at[to],
            dst_ref=recv.at[me],
            send_sem=send_sem.at[to],
            recv_sem=recv_sem.at[me],
            device_id=(to // ny, lax.rem(to, ny)),
            device_id_type=MESH,
        )

    def go(s, _):
        copy_to(s).start()
        return 0

    lax.fori_loop(1, count, go, 0)
    own.wait()

    def arrive(s, _):
        come = lax.rem(me + count - s, count)
        pltpu.make_async_remote_copy(
            src_ref=send.at[come],
            dst_ref=recv.at[come],
            send_sem=send_sem.at[come],
            recv_sem=recv_sem.at[come],
            device_id=(come // ny, lax.rem(come, ny)),
            device_id_type=MESH,
        ).wait_recv()
        return 0

    lax.fori_loop(1, count, arrive, 0)

    tiles = out.shape[1]
    halves = out.shape[2] // LANES
    high_rows = tiles * halves
    high_iota = lax.broadcasted_iota(jnp.int32, (high_rows, LANES), 0).astype(jnp.float32)
    low_iota = lax.broadcasted_iota(jnp.int32, (LANES, LANES), 0).astype(jnp.float32)

    def add(step, total):
        lefts, rights = [], []
        for u in range(unroll):
            blk = recv[step * unroll + u]
            for j in range(cap_rows):
                def row(v):
                    r = v * cap_rows + j
                    return blk[r : r + 1]
                here = high_iota == row(3)
                parts = []
                for c in range(3):
                    value = row(c)
                    top = value.astype(jnp.bfloat16).astype(jnp.float32)
                    parts += [jnp.where(here, top, 0.0), jnp.where(here, value - top, 0.0)]
                lefts.append(jnp.concatenate(parts, axis=0).astype(jnp.bfloat16))
                rights.append(jnp.where(low_iota == row(4), 1.0, 0.0).astype(jnp.bfloat16))
        left = jnp.concatenate(lefts, axis=1)
        right = jnp.concatenate(rights, axis=1)
        return total + lax.dot_general(left, right, NT, preferred_element_type=jnp.float32)

    total = lax.fori_loop(
        0, count // unroll, add, jnp.zeros((6 * high_rows, LANES), jnp.float32)
    )
    for c in range(3):
        for h in range(halves):
            at = 2 * c * high_rows + h * tiles
            out[c, :, h * LANES : (h + 1) * LANES] = (
                total[at : at + tiles] + total[at + high_rows : at + high_rows + tiles]
            )

    def sent(s, _):
        copy_to(s).wait_send()
        return 0

    lax.fori_loop(1, count, sent, 0)


def gather_film(send, nx, ny, cap_rows, tiles):
    count = nx * ny
    return pl.pallas_call(
        functools.partial(film_kernel, nx, ny, cap_rows, 4),
        out_shape=jax.ShapeDtypeStruct((3, tiles, TILE_PIX), jnp.float32),
        in_specs=[pl.BlockSpec(memory_space=pltpu.VMEM)],
        out_specs=pl.BlockSpec(memory_space=pltpu.VMEM),
        scratch_shapes=[
            pltpu.VMEM(send.shape, jnp.float32),
            pltpu.SemaphoreType.DMA((count,)),
            pltpu.SemaphoreType.DMA((count,)),
            pltpu.SemaphoreType.DMA,
        ],
        compiler_params=pltpu.CompilerParams(collective_id=1, has_side_effects=True),
        name="film",
    )(send)


def per_device(
    nx, ny, photon_data, block_counts, gather_offsets, gather_blocks, albedo, gather_pixels, tile_slot
):
    cx, cy, slots = photon_data.shape[1:]
    grid_x, grid_y = cx * nx, cy * ny
    points = gather_offsets.shape[1]
    owners = nx * ny
    tiles = tile_slot.shape[0]
    tiles_dev = tiles // owners
    cap_rows = -(-(3 * points // owners) // LANES)

    live = lax.broadcasted_iota(jnp.int32, (cx, cy, slots), 2) < block_counts[:, :, None]
    first = jnp.where(live, photon_data[0], FAR)

    def edge(x, y):
        a = first[x, y].reshape(1, -1, slots)
        b = photon_data[1:, x, y].reshape(5, -1, slots)
        return jnp.concatenate([a, b], axis=0)

    every = slice(None)
    tail, head = slice(cy - 8, cy), slice(0, 8)
    send = jnp.concatenate(
        [
            edge(cx - 1, every),
            edge(0, every),
            edge(every, cy - 1),
            edge(every, 0),
            edge(cx - 1, tail),
            edge(cx - 1, head),
            edge(0, tail),
            edge(0, head),
        ],
        axis=1,
    )
    halo = exchange_halo(send, nx, ny, cx, cy)

    first_x = lax.axis_index("bx") * cx
    first_y = lax.axis_index("by") * cy
    lx = (gather_blocks // grid_y - first_x + 1) % grid_x
    ly = (gather_blocks % grid_y - first_y + 1) % grid_y
    shift_x = (lx - lx[:1]).astype(jnp.float32)
    shift_y = (ly - ly[:1]).astype(jnp.float32)
    cells = cx * cy
    x_out = (lx == 0) | (lx == cx + 1)
    y_out = (ly == 0) | (ly == cy + 1)
    x_far = (lx == cx + 1).astype(jnp.int32)
    y_far = (ly == cy + 1).astype(jnp.int32)
    corner = 2 * cy + 2 * cx + 16 * x_far + 8 * y_far + 7 * (1 - y_far)
    index = jnp.where(
        x_out,
        jnp.where(y_out, cells + corner, cells + x_far * cy + ly - 1),
        jnp.where(y_out, cells + 2 * cy + y_far * cx + lx - 1, (lx - 1) * cy + ly - 1),
    )
    pts = jnp.concatenate(
        [
            gather_offsets[0:1] - shift_x,
            gather_offsets[1:2] - shift_y,
            gather_offsets[2:3],
            jnp.zeros((7, points), jnp.float32),
        ],
        axis=0,
    )
    tile = gather_pixels // TILE_PIX
    matched = tile[:, None] == jnp.arange(tiles, dtype=jnp.int32)[None, :]
    slot = jnp.sum(jnp.where(matched, tile_slot[None, :], 0), axis=1)
    within = gather_pixels % TILE_PIX
    meta = jnp.stack(
        [slot // tiles_dev, (within // LANES) * tiles_dev + slot % tiles_dev, within % LANES]
    )
    packed = pack_radiance(
        index.reshape(-1), pts, albedo, meta, first.reshape(cells, slots),
        photon_data.reshape(6, cells, slots), halo, owners, cap_rows,
    )
    return gather_film(packed.reshape(owners, -1, LANES), nx, ny, cap_rows, tiles_dev)


def solution(mesh):
    both = ("bx", "by")
    in_specs = (
        P(None, "bx", "by", None), P("bx", "by"), P(None, both), P(None, both),
        P(None, both), P(both), P(),
    )
    return jax.shard_map(
        functools.partial(per_device, mesh.shape["bx"], mesh.shape["by"]),
        mesh=mesh, in_specs=in_specs, out_specs=P(None, both, None), check_vma=False,
    )
```

```python
import functools

import jax
import jax.numpy as jnp
from jax import lax
from jax.experimental import pallas as pl
from jax.experimental.pallas import tpu as pltpu
from jax.sharding import PartitionSpec as P

TILE_PIX = 256
INV_RADIUS_SQ = 4.0
FAR = 1.0e4
LANES = 128
MESH = pl.DeviceIdType.MESH
NT = (((1,), (1,)), ((), ()))
PITCH = LANES + 1


def halo_kernel(nx, ny, cx, cy, send, recv, send_sem, recv_sem):
    ix, iy = lax.axis_index("bx"), lax.axis_index("by")
    right, left = lax.rem(ix + 1, nx), lax.rem(ix + nx - 1, nx)
    up, down = lax.rem(iy + 1, ny), lax.rem(iy + ny - 1, ny)
    peers = [
        (right, iy, 0, cy),
        (left, iy, cy, cy),
        (ix, up, 2 * cy, cx),
        (ix, down, 2 * cy + cx, cx),
        (right, up, 2 * cy + 2 * cx, 8),
        (right, down, 2 * cy + 2 * cx + 8, 8),
        (left, up, 2 * cy + 2 * cx + 16, 8),
        (left, down, 2 * cy + 2 * cx + 24, 8),
    ]
    barrier = pltpu.get_barrier_semaphore()
    for px, py, _, _ in peers:
        pl.semaphore_signal(barrier, inc=1, device_id=(px, py), device_id_type=MESH)
    pl.semaphore_wait(barrier, len(peers))
    copies = []
    for n, (px, py, first, rows) in enumerate(peers):
        part = pl.ds(first, rows)
        copies.append(
            pltpu.make_async_remote_copy(
                src_ref=send.at[:, part],
                dst_ref=recv.at[:, part],
                send_sem=send_sem.at[n],
                recv_sem=recv_sem.at[n],
                device_id=(px, py),
                device_id_type=MESH,
            )
        )
    for n in (2, 3, 0, 1, 4, 5, 6, 7):
        copies[n].start()
    for copy in copies:
        copy.wait()


def exchange_halo(send, nx, ny, cx, cy):
    return pl.pallas_call(
        functools.partial(halo_kernel, nx, ny, cx, cy),
        out_shape=jax.ShapeDtypeStruct(send.shape, jnp.float32),
        in_specs=[pl.BlockSpec(memory_space=pl.ANY)],
        out_specs=pl.BlockSpec(memory_space=pl.ANY),
        scratch_shapes=[pltpu.SemaphoreType.DMA((8,)), pltpu.SemaphoreType.DMA((8,))],
        compiler_params=pltpu.CompilerParams(collective_id=0, has_side_effects=True),
        name="halo",
    )(send)


def radiance_kernel(
    cells, rows, owners, cap_rows,
    idx, pts, alb, meta, first, rest, halo, out,
    table, stage, wide, acc, packed, tri, spread, sems,
):
    listed = 4
    points = pts.shape[1]
    fills = [pltpu.make_async_copy(first, table.at[pl.ds(0, cells), 0], sems.at[0])]
    for c in range(1, 6):
        fills.append(pltpu.make_async_copy(rest.at[c], table.at[pl.ds(0, cells), c], sems.at[c]))
    for c in range(6):
        fills.append(
            pltpu.make_async_copy(
                halo.at[c], table.at[pl.ds(cells, rows - cells), c], sems.at[6 + c]
            )
        )
    for fill in fills:
        fill.start()
    a = lax.broadcasted_iota(jnp.int32, (LANES, LANES), 0)
    b = lax.broadcasted_iota(jnp.int32, (LANES, LANES), 1)
    tri[...] = jnp.where(a < b, 1.0, 0.0).astype(jnp.bfloat16)
    a = lax.broadcasted_iota(jnp.int32, spread.shape, 0)
    b = lax.broadcasted_iota(jnp.int32, spread.shape, 1)
    spread[...] = jnp.where(a % 16 == b // LANES, 1.0, 0.0).astype(jnp.bfloat16)
    packed[...] = jnp.zeros_like(packed)
    own_iota = lax.broadcasted_iota(jnp.int32, (owners, LANES), 0)
    cap_iota = lax.broadcasted_iota(jnp.int32, (cap_rows * LANES, LANES), 0).astype(jnp.float32)
    for fill in fills:
        fill.wait()

    def block(blk, carry):
        base = pl.multiple_of(blk * LANES, LANES)
        span = pl.ds(base, LANES)
        value = pts[:, span]
        parts = []
        for _ in range(3):
            high = value.astype(jnp.bfloat16)
            parts.append(high)
            value = value - high.astype(jnp.float32)
        wide[...] = lax.dot_general(
            jnp.concatenate(parts, axis=0), spread[...], (((0,), (0,)), ((), ())),
            preferred_element_type=jnp.float32,
        )
        for p in range(LANES):
            for k in range(listed):
                stage[pl.ds(k * 8 * PITCH + p, 8, stride=PITCH), :] = table[
                    idx[k * points + base + p]
                ]
        for q in range(LANES // 8):
            place = slice(q * 8, q * 8 + 8)

            def column(n):
                return wide[place, n * LANES : (n + 1) * LANES]

            oz = column(8)
            totals = [None] * 3
            for k in range(listed):
                def chan(c):
                    return stage[pl.ds((k * 8 + c) * PITCH + q * 8, 8), :]

                dx = chan(0) - column(k)
                dy = chan(1) - column(4 + k)
                dz = chan(2) - oz
                d2 = dx * dx + dy * dy + dz * dz
                w = jnp.maximum(1.0 - d2 * INV_RADIUS_SQ, 0.0)
                for c in range(3):
                    term = w * chan(3 + c)
                    totals[c] = term if k == 0 else totals[c] + term
            for c in range(3):
                acc[c, place, :] = totals[c]
        own = meta[0:1, span]
        mine = own_iota == own
        hot = jnp.where(mine, 1.0, 0.0)
        before = jnp.dot(hot.astype(jnp.bfloat16), tri[...], preferred_element_type=jnp.float32)
        rank = jnp.sum(jnp.where(mine, before + carry, 0.0), axis=0, keepdims=True)
        values = []
        for c in range(3):
            rad = jnp.sum(acc[c].T, axis=0, keepdims=True) * alb[c : c + 1, span]
            high = rad.astype(jnp.bfloat16).astype(jnp.float32)
            values += [high, rad - high]
        values += [meta[1:2, span].astype(jnp.float32), meta[2:3, span].astype(jnp.float32)]
        left = jnp.concatenate(
            [jnp.where(mine, v, 0.0).astype(jnp.bfloat16) for v in values], axis=0
        )
        right = jnp.where(cap_iota == rank, 1.0, 0.0).astype(jnp.bfloat16)
        packed[...] += lax.dot_general(left, right, NT, preferred_element_type=jnp.float32)
        return carry + jnp.sum(hot, axis=1, keepdims=True)

    lax.fori_loop(0, points // LANES, block, jnp.zeros((owners, 1), jnp.float32))
    pitch = out.shape[0] // owners

    def part(v, j):
        return packed[pl.ds(v * owners, owners), pl.ds(j * LANES, LANES)]

    for j in range(cap_rows):
        for c in range(3):
            out[pl.ds(c * cap_rows + j, owners, stride=pitch), :] = part(2 * c, j) + part(2 * c + 1, j)
        out[pl.ds(3 * cap_rows + j, owners, stride=pitch), :] = part(6, j)
        out[pl.ds(4 * cap_rows + j, owners, stride=pitch), :] = part(7, j)
    for r in range(5 * cap_rows, pitch):
        out[pl.ds(r, owners, stride=pitch), :] = jnp.zeros((owners, LANES), jnp.float32)


def pack_radiance(idx, pts, alb, meta, first, photons, halo, owners, cap_rows):
    cells = first.shape[0]
    rows = cells + halo.shape[1]
    pitch = -(-5 * cap_rows // 8) * 8
    vm = pl.BlockSpec(memory_space=pltpu.VMEM)
    hb = pl.BlockSpec(memory_space=pl.ANY)
    return pl.pallas_call(
        functools.partial(radiance_kernel, cells, rows, owners, cap_rows),
        out_shape=jax.ShapeDtypeStruct((owners * pitch, LANES), jnp.float32),
        in_specs=[pl.BlockSpec(memory_space=pltpu.SMEM), vm, vm, vm, hb, hb, hb],
        out_specs=vm,
        scratch_shapes=[
            pltpu.VMEM((rows, 8, LANES), jnp.float32),
            pltpu.VMEM((4 * 8 * PITCH + 8, LANES), jnp.float32),
            pltpu.VMEM((LANES, 9 * LANES), jnp.float32),
            pltpu.VMEM((3, LANES, LANES), jnp.float32),
            pltpu.VMEM((8 * owners, cap_rows * LANES), jnp.float32),
            pltpu.VMEM((LANES, LANES), jnp.bfloat16),
            pltpu.VMEM((48, 9 * LANES), jnp.bfloat16),
            pltpu.SemaphoreType.DMA((12,)),
        ],
        name="radiance",
    )(idx, pts, alb, meta, first, photons, halo)


def film_kernel(nx, ny, cap_rows, unroll, send, out, recv, send_sem, recv_sem, own_sem):
    count = nx * ny
    ix, iy = lax.axis_index("bx"), lax.axis_index("by")
    me = ix * ny + iy
    barrier = pltpu.get_barrier_semaphore()

    def greet(s, _):
        to = lax.rem(me + s, count)
        pl.semaphore_signal(
            barrier, inc=1, device_id=(to // ny, lax.rem(to, ny)), device_id_type=MESH
        )
        return 0

    lax.fori_loop(1, count, greet, 0)
    own = pltpu.make_async_copy(send.at[me], recv.at[me], own_sem)
    own.start()
    pl.semaphore_wait(barrier, count - 1)

    def copy_to(s):
        to = lax.rem(me + s, count)
        return pltpu.make_async_remote_copy(
            src_ref=send.at[to],
            dst_ref=recv.at[me],
            send_sem=send_sem.at[to],
            recv_sem=recv_sem.at[me],
            device_id=(to // ny, lax.rem(to, ny)),
            device_id_type=MESH,
        )

    def go(s, _):
        copy_to(s).start()
        return 0

    lax.fori_loop(1, count, go, 0)
    own.wait()

    def arrive(s, _):
        come = lax.rem(me + count - s, count)
        pltpu.make_async_remote_copy(
            src_ref=send.at[come],
            dst_ref=recv.at[come],
            send_sem=send_sem.at[come],
            recv_sem=recv_sem.at[come],
            device_id=(come // ny, lax.rem(come, ny)),
            device_id_type=MESH,
        ).wait_recv()
        return 0

    lax.fori_loop(1, count, arrive, 0)

    tiles = out.shape[1]
    halves = out.shape[2] // LANES
    high_rows = tiles * halves
    high_iota = lax.broadcasted_iota(jnp.int32, (high_rows, LANES), 0).astype(jnp.float32)
    low_iota = lax.broadcasted_iota(jnp.int32, (LANES, LANES), 0).astype(jnp.float32)

    def add(step, total):
        lefts, rights = [], []
        for u in range(unroll):
            blk = recv[step * unroll + u]
            for j in range(cap_rows):
                def row(v):
                    r = v * cap_rows + j
                    return blk[r : r + 1]
                here = high_iota == row(3)
                parts = []
                for c in range(3):
                    value = row(c)
                    top = value.astype(jnp.bfloat16).astype(jnp.float32)
                    parts += [jnp.where(here, top, 0.0), jnp.where(here, value - top, 0.0)]
                lefts.append(jnp.concatenate(parts, axis=0).astype(jnp.bfloat16))
                rights.append(jnp.where(low_iota == row(4), 1.0, 0.0).astype(jnp.bfloat16))
        left = jnp.concatenate(lefts, axis=1)
        right = jnp.concatenate(rights, axis=1)
        return total + lax.dot_general(left, right, NT, preferred_element_type=jnp.float32)

    total = lax.fori_loop(
        0, count // unroll, add, jnp.zeros((6 * high_rows, LANES), jnp.float32)
    )
    for c in range(3):
        for h in range(halves):
            at = 2 * c * high_rows + h * tiles
            out[c, :, h * LANES : (h + 1) * LANES] = (
                total[at : at + tiles] + total[at + high_rows : at + high_rows + tiles]
            )

    def sent(s, _):
        copy_to(s).wait_send()
        return 0

    lax.fori_loop(1, count, sent, 0)


def gather_film(send, nx, ny, cap_rows, tiles):
    count = nx * ny
    return pl.pallas_call(
        functools.partial(film_kernel, nx, ny, cap_rows, 4),
        out_shape=jax.ShapeDtypeStruct((3, tiles, TILE_PIX), jnp.float32),
        in_specs=[pl.BlockSpec(memory_space=pltpu.VMEM)],
        out_specs=pl.BlockSpec(memory_space=pltpu.VMEM),
        scratch_shapes=[
            pltpu.VMEM(send.shape, jnp.float32),
            pltpu.SemaphoreType.DMA((count,)),
            pltpu.SemaphoreType.DMA((count,)),
            pltpu.SemaphoreType.DMA,
        ],
        compiler_params=pltpu.CompilerParams(collective_id=1, has_side_effects=True),
        name="film",
    )(send)


def per_device(
    nx, ny, photon_data, block_counts, gather_offsets, gather_blocks, albedo, gather_pixels, tile_slot
):
    cx, cy, slots = photon_data.shape[1:]
    grid_x, grid_y = cx * nx, cy * ny
    points = gather_offsets.shape[1]
    owners = nx * ny
    tiles = tile_slot.shape[0]
    tiles_dev = tiles // owners
    cap_rows = -(-(3 * points // owners) // LANES)

    live = lax.broadcasted_iota(jnp.int32, (cx, cy, slots), 2) < block_counts[:, :, None]
    first = jnp.where(live, photon_data[0], FAR)

    def edge(x, y):
        a = first[x, y].reshape(1, -1, slots)
        b = photon_data[1:, x, y].reshape(5, -1, slots)
        return jnp.concatenate([a, b], axis=0)

    every = slice(None)
    tail, head = slice(cy - 8, cy), slice(0, 8)
    send = jnp.concatenate(
        [
            edge(cx - 1, every),
            edge(0, every),
            edge(every, cy - 1),
            edge(every, 0),
            edge(cx - 1, tail),
            edge(cx - 1, head),
            edge(0, tail),
            edge(0, head),
        ],
        axis=1,
    )
    halo = exchange_halo(send, nx, ny, cx, cy)

    first_x = lax.axis_index("bx") * cx
    first_y = lax.axis_index("by") * cy
    lx = (gather_blocks // grid_y - first_x + 1) % grid_x
    ly = (gather_blocks % grid_y - first_y + 1) % grid_y
    shift_x = (lx - lx[:1]).astype(jnp.float32)
    shift_y = (ly - ly[:1]).astype(jnp.float32)
    cells = cx * cy
    x_out = (lx == 0) | (lx == cx + 1)
    y_out = (ly == 0) | (ly == cy + 1)
    x_far = (lx == cx + 1).astype(jnp.int32)
    y_far = (ly == cy + 1).astype(jnp.int32)
    corner = 2 * cy + 2 * cx + 16 * x_far + 8 * y_far + 7 * (1 - y_far)
    index = jnp.where(
        x_out,
        jnp.where(y_out, cells + corner, cells + x_far * cy + ly - 1),
        jnp.where(y_out, cells + 2 * cy + y_far * cx + lx - 1, (lx - 1) * cy + ly - 1),
    )
    pts = jnp.concatenate(
        [
            gather_offsets[0:1] - shift_x,
            gather_offsets[1:2] - shift_y,
            gather_offsets[2:3],
            jnp.zeros((7, points), jnp.float32),
        ],
        axis=0,
    )
    tile = gather_pixels // TILE_PIX
    matched = tile[:, None] == jnp.arange(tiles, dtype=jnp.int32)[None, :]
    slot = jnp.sum(jnp.where(matched, tile_slot[None, :], 0), axis=1)
    within = gather_pixels % TILE_PIX
    meta = jnp.stack(
        [slot // tiles_dev, (within // LANES) * tiles_dev + slot % tiles_dev, within % LANES]
    )
    packed = pack_radiance(
        index.reshape(-1), pts, albedo, meta, first.reshape(cells, slots),
        photon_data.reshape(6, cells, slots), halo, owners, cap_rows,
    )
    return gather_film(packed.reshape(owners, -1, LANES), nx, ny, cap_rows, tiles_dev)


def solution(mesh):
    both = ("bx", "by")
    in_specs = (
        P(None, "bx", "by", None), P("bx", "by"), P(None, both), P(None, both),
        P(None, both), P(both), P(),
    )
    return jax.shard_map(
        functools.partial(per_device, mesh.shape["bx"], mesh.shape["by"]),
        mesh=mesh, in_specs=in_specs, out_specs=P(None, both, None), check_vma=False,
    )
```

```python
import functools

import jax
import jax.numpy as jnp
from jax import lax
from jax.experimental import pallas as pl
from jax.experimental.pallas import tpu as pltpu
from jax.sharding import PartitionSpec as P

TILE_PIX = 256
INV_RADIUS_SQ = 4.0
FAR = 1.0e4
LANES = 128
MESH = pl.DeviceIdType.MESH
NT = (((1,), (1,)), ((), ()))
PITCH = LANES + 1


def halo_kernel(nx, ny, cx, cy, first, photons, recv, send, send_sem, recv_sem, edge_sem):
    ix, iy = lax.axis_index("bx"), lax.axis_index("by")
    right, left = lax.rem(ix + 1, nx), lax.rem(ix + nx - 1, nx)
    up, down = lax.rem(iy + 1, ny), lax.rem(iy + ny - 1, ny)
    peers = [
        (right, iy, 0, cy),
        (left, iy, cy, cy),
        (ix, up, 2 * cy, cx),
        (ix, down, 2 * cy + cx, cx),
        (right, up, 2 * cy + 2 * cx, 8),
        (right, down, 2 * cy + 2 * cx + 8, 8),
        (left, up, 2 * cy + 2 * cx + 16, 8),
        (left, down, 2 * cy + 2 * cx + 24, 8),
    ]
    every, tail, head = pl.ds(0, cy), pl.ds(cy - 8, 8), pl.ds(0, 8)
    wide = pl.ds(0, cx)
    cuts = [
        (cx - 1, every), (0, every), (wide, cy - 1), (wide, 0),
        (cx - 1, tail), (cx - 1, head), (0, tail), (0, head),
    ]
    edges = []
    for n, (x, y) in enumerate(cuts):
        part = pl.ds(peers[n][2], peers[n][3])
        edges.append(
            pltpu.make_async_copy(
                photons.at[pl.ds(1, 5), x, y], send.at[pl.ds(1, 5), part], edge_sem.at[2 * n]
            )
        )
        edges.append(
            pltpu.make_async_copy(first.at[x, y], send.at[0, part], edge_sem.at[2 * n + 1])
        )
    for n in (2, 3, 0, 1, 4, 5, 6, 7):
        edges[2 * n].start()
        edges[2 * n + 1].start()
    barrier = pltpu.get_barrier_semaphore()
    for px, py, _, _ in peers:
        pl.semaphore_signal(barrier, inc=1, device_id=(px, py), device_id_type=MESH)
    pl.semaphore_wait(barrier, len(peers))
    copies = []
    for n, (px, py, first, rows) in enumerate(peers):
        part = pl.ds(first, rows)
        copies.append(
            pltpu.make_async_remote_copy(
                src_ref=send.at[:, part],
                dst_ref=recv.at[:, part],
                send_sem=send_sem.at[n],
                recv_sem=recv_sem.at[n],
                device_id=(px, py),
                device_id_type=MESH,
            )
        )
    for n in (2, 3, 0, 1, 4, 5, 6, 7):
        edges[2 * n].wait()
        edges[2 * n + 1].wait()
        copies[n].start()
    for copy in copies:
        copy.wait()


def exchange_halo(first, photons, nx, ny, cx, cy):
    shape = (6, 2 * cy + 2 * cx + 32, photons.shape[3])
    return pl.pallas_call(
        functools.partial(halo_kernel, nx, ny, cx, cy),
        out_shape=jax.ShapeDtypeStruct(shape, jnp.float32),
        in_specs=[pl.BlockSpec(memory_space=pl.ANY)] * 2,
        out_specs=pl.BlockSpec(memory_space=pl.ANY),
        scratch_shapes=[
            pltpu.VMEM(shape, jnp.float32),
            pltpu.SemaphoreType.DMA((8,)),
            pltpu.SemaphoreType.DMA((8,)),
            pltpu.SemaphoreType.DMA((16,)),
        ],
        compiler_params=pltpu.CompilerParams(collective_id=0, has_side_effects=True),
        name="halo",
    )(first, photons)


def radiance_kernel(
    cells, rows, owners, cap_rows,
    idx, pts, alb, meta, first, rest, halo, out,
    table, stage, wide, acc, packed, tri, spread, sems,
):
    listed = 4
    points = pts.shape[1]
    fills = [pltpu.make_async_copy(first, table.at[pl.ds(0, cells), 0], sems.at[0])]
    for c in range(1, 6):
        fills.append(pltpu.make_async_copy(rest.at[c], table.at[pl.ds(0, cells), c], sems.at[c]))
    for c in range(6):
        fills.append(
            pltpu.make_async_copy(
                halo.at[c], table.at[pl.ds(cells, rows - cells), c], sems.at[6 + c]
            )
        )
    for fill in fills:
        fill.start()
    a = lax.broadcasted_iota(jnp.int32, (LANES, LANES), 0)
    b = lax.broadcasted_iota(jnp.int32, (LANES, LANES), 1)
    tri[...] = jnp.where(a < b, 1.0, 0.0).astype(jnp.bfloat16)
    a = lax.broadcasted_iota(jnp.int32, spread.shape, 0)
    b = lax.broadcasted_iota(jnp.int32, spread.shape, 1)
    spread[...] = jnp.where(a % 16 == b // LANES, 1.0, 0.0).astype(jnp.bfloat16)
    packed[...] = jnp.zeros_like(packed)
    own_iota = lax.broadcasted_iota(jnp.int32, (owners, LANES), 0)
    cap_iota = lax.broadcasted_iota(jnp.int32, (cap_rows * LANES, LANES), 0).astype(jnp.float32)
    for fill in fills:
        fill.wait()

    def block(blk, carry):
        base = pl.multiple_of(blk * LANES, LANES)
        span = pl.ds(base, LANES)
        value = pts[:, span]
        parts = []
        for _ in range(3):
            high = value.astype(jnp.bfloat16)
            parts.append(high)
            value = value - high.astype(jnp.float32)
        wide[...] = lax.dot_general(
            jnp.concatenate(parts, axis=0), spread[...], (((0,), (0,)), ((), ())),
            preferred_element_type=jnp.float32,
        )
        for p in range(LANES):
            for k in range(listed):
                stage[pl.ds(k * 8 * PITCH + p, 8, stride=PITCH), :] = table[
                    idx[k * points + base + p]
                ]
        for q in range(LANES // 8):
            place = slice(q * 8, q * 8 + 8)

            def column(n):
                return wide[place, n * LANES : (n + 1) * LANES]

            oz = column(8)
            totals = [None] * 3
            for k in range(listed):
                def chan(c):
                    return stage[pl.ds((k * 8 + c) * PITCH + q * 8, 8), :]

                dx = chan(0) - column(k)
                dy = chan(1) - column(4 + k)
                dz = chan(2) - oz
                d2 = dx * dx + dy * dy + dz * dz
                w = jnp.maximum(1.0 - d2 * INV_RADIUS_SQ, 0.0)
                for c in range(3):
                    term = w * chan(3 + c)
                    totals[c] = term if k == 0 else totals[c] + term
            for c in range(3):
                acc[c, place, :] = totals[c]
        own = meta[0:1, span]
        mine = own_iota == own
        hot = jnp.where(mine, 1.0, 0.0)
        before = jnp.dot(hot.astype(jnp.bfloat16), tri[...], preferred_element_type=jnp.float32)
        rank = jnp.sum(jnp.where(mine, before + carry, 0.0), axis=0, keepdims=True)
        values = []
        for c in range(3):
            rad = jnp.sum(acc[c].T, axis=0, keepdims=True) * alb[c : c + 1, span]
            high = rad.astype(jnp.bfloat16).astype(jnp.float32)
            values += [high, rad - high]
        values += [meta[1:2, span].astype(jnp.float32), meta[2:3, span].astype(jnp.float32)]
        left = jnp.concatenate(
            [jnp.where(mine, v, 0.0).astype(jnp.bfloat16) for v in values], axis=0
        )
        right = jnp.where(cap_iota == rank, 1.0, 0.0).astype(jnp.bfloat16)
        packed[...] += lax.dot_general(left, right, NT, preferred_element_type=jnp.float32)
        return carry + jnp.sum(hot, axis=1, keepdims=True)

    lax.fori_loop(0, points // LANES, block, jnp.zeros((owners, 1), jnp.float32))
    pitch = out.shape[0] // owners

    def part(v, j):
        return packed[pl.ds(v * owners, owners), pl.ds(j * LANES, LANES)]

    for j in range(cap_rows):
        for c in range(3):
            out[pl.ds(c * cap_rows + j, owners, stride=pitch), :] = part(2 * c, j) + part(2 * c + 1, j)
        out[pl.ds(3 * cap_rows + j, owners, stride=pitch), :] = part(6, j)
        out[pl.ds(4 * cap_rows + j, owners, stride=pitch), :] = part(7, j)
    for r in range(5 * cap_rows, pitch):
        out[pl.ds(r, owners, stride=pitch), :] = jnp.zeros((owners, LANES), jnp.float32)


def pack_radiance(idx, pts, alb, meta, first, photons, halo, owners, cap_rows):
    cells = first.shape[0]
    rows = cells + halo.shape[1]
    pitch = -(-5 * cap_rows // 8) * 8
    vm = pl.BlockSpec(memory_space=pltpu.VMEM)
    hb = pl.BlockSpec(memory_space=pl.ANY)
    return pl.pallas_call(
        functools.partial(radiance_kernel, cells, rows, owners, cap_rows),
        out_shape=jax.ShapeDtypeStruct((owners * pitch, LANES), jnp.float32),
        in_specs=[pl.BlockSpec(memory_space=pltpu.SMEM), vm, vm, vm, hb, hb, hb],
        out_specs=vm,
        scratch_shapes=[
            pltpu.VMEM((rows, 8, LANES), jnp.float32),
            pltpu.VMEM((4 * 8 * PITCH + 8, LANES), jnp.float32),
            pltpu.VMEM((LANES, 9 * LANES), jnp.float32),
            pltpu.VMEM((3, LANES, LANES), jnp.float32),
            pltpu.VMEM((8 * owners, cap_rows * LANES), jnp.float32),
            pltpu.VMEM((LANES, LANES), jnp.bfloat16),
            pltpu.VMEM((48, 9 * LANES), jnp.bfloat16),
            pltpu.SemaphoreType.DMA((12,)),
        ],
        name="radiance",
    )(idx, pts, alb, meta, first, photons, halo)


def film_kernel(nx, ny, cap_rows, unroll, send, out, recv, send_sem, recv_sem, own_sem):
    count = nx * ny
    ix, iy = lax.axis_index("bx"), lax.axis_index("by")
    me = ix * ny + iy
    barrier = pltpu.get_barrier_semaphore()

    def greet(s, _):
        to = lax.rem(me + s, count)
        pl.semaphore_signal(
            barrier, inc=1, device_id=(to // ny, lax.rem(to, ny)), device_id_type=MESH
        )
        return 0

    lax.fori_loop(1, count, greet, 0)
    own = pltpu.make_async_copy(send.at[me], recv.at[me], own_sem)
    own.start()
    pl.semaphore_wait(barrier, count - 1)

    def copy_to(s):
        to = lax.rem(me + s, count)
        return pltpu.make_async_remote_copy(
            src_ref=send.at[to],
            dst_ref=recv.at[me],
            send_sem=send_sem.at[to],
            recv_sem=recv_sem.at[me],
            device_id=(to // ny, lax.rem(to, ny)),
            device_id_type=MESH,
        )

    def go(s, _):
        copy_to(s).start()
        return 0

    lax.fori_loop(1, count, go, 0)
    own.wait()

    def arrive(s):
        come = lax.rem(me + count - s, count)

        @pl.when(s > 0)
        def _():
            pltpu.make_async_remote_copy(
                src_ref=send.at[come],
                dst_ref=recv.at[come],
                send_sem=send_sem.at[come],
                recv_sem=recv_sem.at[come],
                device_id=(come // ny, lax.rem(come, ny)),
                device_id_type=MESH,
            ).wait_recv()

        return come

    tiles = out.shape[1]
    halves = out.shape[2] // LANES
    high_rows = tiles * halves
    high_iota = lax.broadcasted_iota(jnp.int32, (high_rows, LANES), 0).astype(jnp.float32)
    low_iota = lax.broadcasted_iota(jnp.int32, (LANES, LANES), 0).astype(jnp.float32)

    def add(step, total):
        lefts, rights = [], []
        sources = [arrive(step * unroll + u) for u in range(unroll)]
        for come in sources:
            blk = recv[come]
            for j in range(cap_rows):
                def row(v):
                    r = v * cap_rows + j
                    return blk[r : r + 1]
                here = high_iota == row(3)
                parts = []
                for c in range(3):
                    value = row(c)
                    top = value.astype(jnp.bfloat16).astype(jnp.float32)
                    parts += [jnp.where(here, top, 0.0), jnp.where(here, value - top, 0.0)]
                lefts.append(jnp.concatenate(parts, axis=0).astype(jnp.bfloat16))
                rights.append(jnp.where(low_iota == row(4), 1.0, 0.0).astype(jnp.bfloat16))
        left = jnp.concatenate(lefts, axis=1)
        right = jnp.concatenate(rights, axis=1)
        return total + lax.dot_general(left, right, NT, preferred_element_type=jnp.float32)

    total = lax.fori_loop(
        0, count // unroll, add, jnp.zeros((6 * high_rows, LANES), jnp.float32)
    )
    for c in range(3):
        for h in range(halves):
            at = 2 * c * high_rows + h * tiles
            out[c, :, h * LANES : (h + 1) * LANES] = (
                total[at : at + tiles] + total[at + high_rows : at + high_rows + tiles]
            )

    def sent(s, _):
        copy_to(s).wait_send()
        return 0

    lax.fori_loop(1, count, sent, 0)


def gather_film(send, nx, ny, cap_rows, tiles):
    count = nx * ny
    return pl.pallas_call(
        functools.partial(film_kernel, nx, ny, cap_rows, 4),
        out_shape=jax.ShapeDtypeStruct((3, tiles, TILE_PIX), jnp.float32),
        in_specs=[pl.BlockSpec(memory_space=pltpu.VMEM)],
        out_specs=pl.BlockSpec(memory_space=pltpu.VMEM),
        scratch_shapes=[
            pltpu.VMEM(send.shape, jnp.float32),
            pltpu.SemaphoreType.DMA((count,)),
            pltpu.SemaphoreType.DMA((count,)),
            pltpu.SemaphoreType.DMA,
        ],
        compiler_params=pltpu.CompilerParams(collective_id=1, has_side_effects=True),
        name="film",
    )(send)


def per_device(
    nx, ny, photon_data, block_counts, gather_offsets, gather_blocks, albedo, gather_pixels, tile_slot
):
    cx, cy, slots = photon_data.shape[1:]
    grid_x, grid_y = cx * nx, cy * ny
    points = gather_offsets.shape[1]
    owners = nx * ny
    tiles = tile_slot.shape[0]
    tiles_dev = tiles // owners
    cap_rows = -(-(3 * points // owners) // LANES)

    live = lax.broadcasted_iota(jnp.int32, (cx, cy, slots), 2) < block_counts[:, :, None]
    first = jnp.where(live, photon_data[0], FAR)

    first = lax.optimization_barrier(first)
    halo = exchange_halo(first, photon_data, nx, ny, cx, cy)

    first_x = lax.axis_index("bx") * cx
    first_y = lax.axis_index("by") * cy
    lx = (gather_blocks // grid_y - first_x + 1) % grid_x
    ly = (gather_blocks % grid_y - first_y + 1) % grid_y
    shift_x = (lx - lx[:1]).astype(jnp.float32)
    shift_y = (ly - ly[:1]).astype(jnp.float32)
    cells = cx * cy
    x_out = (lx == 0) | (lx == cx + 1)
    y_out = (ly == 0) | (ly == cy + 1)
    x_far = (lx == cx + 1).astype(jnp.int32)
    y_far = (ly == cy + 1).astype(jnp.int32)
    corner = 2 * cy + 2 * cx + 16 * x_far + 8 * y_far + 7 * (1 - y_far)
    index = jnp.where(
        x_out,
        jnp.where(y_out, cells + corner, cells + x_far * cy + ly - 1),
        jnp.where(y_out, cells + 2 * cy + y_far * cx + lx - 1, (lx - 1) * cy + ly - 1),
    )
    pts = jnp.concatenate(
        [
            gather_offsets[0:1] - shift_x,
            gather_offsets[1:2] - shift_y,
            gather_offsets[2:3],
            jnp.zeros((7, points), jnp.float32),
        ],
        axis=0,
    )
    tile = gather_pixels // TILE_PIX
    matched = tile[:, None] == jnp.arange(tiles, dtype=jnp.int32)[None, :]
    slot = jnp.sum(jnp.where(matched, tile_slot[None, :], 0), axis=1)
    within = gather_pixels % TILE_PIX
    meta = jnp.stack(
        [slot // tiles_dev, (within // LANES) * tiles_dev + slot % tiles_dev, within % LANES]
    )
    packed = pack_radiance(
        index.reshape(-1), pts, albedo, meta, first.reshape(cells, slots),
        photon_data.reshape(6, cells, slots), halo, owners, cap_rows,
    )
    return gather_film(packed.reshape(owners, -1, LANES), nx, ny, cap_rows, tiles_dev)


def solution(mesh):
    both = ("bx", "by")
    in_specs = (
        P(None, "bx", "by", None), P("bx", "by"), P(None, both), P(None, both),
        P(None, both), P(both), P(),
    )
    return jax.shard_map(
        functools.partial(per_device, mesh.shape["bx"], mesh.shape["by"]),
        mesh=mesh, in_specs=in_specs, out_specs=P(None, both, None), check_vma=False,
    )
```
